8 devices in a mesh: rep: 2 (over z, y), data: 4 (over x, core).
Axes of the slice: x: 2, y: 2, z: 1, core: 2. Of those that a mesh axis runs over, the one named last changes fastest.
Arguments:
- x_in: bfloat16 [128, 32, 512], P(('rep', 'data'))
- d_out: float32 [128, 32, 512], P(('rep', 'data'))
- weights: bfloat16 [8, 1024, 2048], replicated
- biases: float32 [8, 2048], replicated
Outputs:
- output 1: float32 [8, 1024, 2048], replicated
- output 2: float32 [8, 2048], replicated
- output 3: float32 [128, 32, 512], P(('rep', 'data'))
All inputs are finite; a program needn't handle non-finite values.
Results may differ from the reference program's by a relative error of at most 0.00553299.
Values are sent between devices in bfloat16 or wider.
A program may use at most 1 GiB of HBM per device.

```python
import jax
import jax.numpy as jnp
from jax import lax

HIDDEN = 512
LAYERS = 8
BATCH = 128
SEQ = 32
BLOCK_ROWS = 16
NUM_BLOCKS = BATCH // BLOCK_ROWS


def setup_inputs(seed: int = 0) -> dict:
    key = jax.random.key(seed)
    k_x, k_dy, k_w, k_b = jax.random.split(key, 4)
    x_in = jax.random.normal(k_x, (BATCH, SEQ, HIDDEN), jnp.float32).astype(jnp.bfloat16)
    d_out = jax.random.normal(k_dy, (BATCH, SEQ, HIDDEN), jnp.float32)
    weights = (jax.random.normal(k_w, (LAYERS, 2 * HIDDEN, 4 * HIDDEN), jnp.float32) * (2 * HIDDEN) ** -0.5).astype(jnp.bfloat16)
    gate_shift = jnp.concatenate([jnp.zeros((HIDDEN,), jnp.float32), jnp.ones((HIDDEN,), jnp.float32), jnp.zeros((2 * HIDDEN,), jnp.float32)])
    biases = 0.5 * jax.random.normal(k_b, (LAYERS, 4 * HIDDEN), jnp.float32) + gate_shift
    return {'x_in': x_in, 'd_out': d_out, 'weights': weights, 'biases': biases}


def gate_values(z_all):
    hidden = z_all.shape[-1] // 4
    return (jax.nn.sigmoid(z_all[:, :hidden]), jax.nn.sigmoid(z_all[:, hidden:2 * hidden]),
            jnp.tanh(z_all[:, 2 * hidden:3 * hidden]), jax.nn.sigmoid(z_all[:, 3 * hidden:]))


def layer_forward(x_seq, w_layer, b_layer):
    w_rec = w_layer[HIDDEN:]
    x_proj = jnp.einsum('tbh,hg->tbg', x_seq.astype(jnp.float32), w_layer[:HIDDEN].astype(jnp.float32)) + b_layer

    def time_step(carry_in, step_in):
        h_prev, c_prev = carry_in
        z_in, x_t = step_in
        z_all = z_in + jnp.dot(h_prev, w_rec, preferred_element_type=jnp.float32)
        in_g, fg_g, cand_g, out_g = gate_values(z_all)
        c_new = fg_g * c_prev + in_g * cand_g
        h_new = out_g * jnp.tanh(c_new)
        h_low = h_new.astype(jnp.bfloat16)
        y_t = (h_new + x_t.astype(jnp.float32)).astype(jnp.bfloat16)
        return (h_low, c_new), (z_all, c_prev, h_low, y_t)

    init_state = (jnp.zeros((BLOCK_ROWS, HIDDEN), jnp.bfloat16), jnp.zeros((BLOCK_ROWS, HIDDEN), jnp.float32))
    _, (z_seq, c_prev_seq, h_seq, y_seq) = lax.scan(time_step, init_state, (x_proj, x_seq))
    return y_seq, (z_seq, c_prev_seq, h_seq)


def layer_backward(dy_seq, x_seq, w_layer, z_seq, c_prev_seq, h_seq):
    w_rec = w_layer[HIDDEN:]

    def time_step(carry_in, step_in):
        dh_rec, dc_next = carry_in
        dy_t, z_all, c_prev = step_in
        in_g, fg_g, cand_g, out_g = gate_values(z_all)
        tanh_c = jnp.tanh(fg_g * c_prev + in_g * cand_g)
        dh_tot = dy_t + dh_rec
        dc_tot = dc_next + dh_tot * out_g * (1.0 - tanh_c * tanh_c)
        dz_all = jnp.concatenate([dc_tot * cand_g * in_g * (1.0 - in_g),
                                  dc_tot * c_prev * fg_g * (1.0 - fg_g),
                                  dc_tot * in_g * (1.0 - cand_g * cand_g),
                                  dh_tot * tanh_c * out_g * (1.0 - out_g)], axis=-1)
        dz_low = dz_all.astype(jnp.bfloat16)
        dh_new = jnp.dot(dz_low, w_rec.T, preferred_element_type=jnp.float32)
        return (dh_new, dc_tot * fg_g), (dz_low, jnp.sum(dz_all, axis=0))

    zero_state = jnp.zeros((BLOCK_ROWS, HIDDEN), jnp.float32)
    _, (dz_seq, db_steps) = lax.scan(time_step, (zero_state, zero_state), (dy_seq, z_seq, c_prev_seq), reverse=True)
    dz_wide = dz_seq.astype(jnp.float32)
    dx_seq = dy_seq + jnp.einsum('tbg,hg->tbh', dz_wide, w_layer[:HIDDEN].astype(jnp.float32))
    dw_in = jnp.einsum('tbh,tbg->hg', x_seq.astype(jnp.float32), dz_wide)
    dw_rec = jnp.einsum('tbh,tbg->hg', h_seq[:-1].astype(jnp.float32), dz_wide[1:])
    return dx_seq, jnp.concatenate([dw_in, dw_rec], axis=0), jnp.sum(db_steps, axis=0)


def block_grads(x_blk, dy_blk, weights, biases):
    def forward_layer(x_cur, layer_params):
        y_seq, saved_acts = layer_forward(x_cur, layer_params[0], layer_params[1])
        return y_seq, (x_cur,) + saved_acts

    _, stored = lax.scan(forward_layer, jnp.swapaxes(x_blk, 0, 1), (weights, biases))

    def backward_layer(dy_cur, layer_data):
        w_layer, x_cur, z_seq, c_prev_seq, h_seq = layer_data
        dx_seq, dw_layer, db_layer = layer_backward(dy_cur, x_cur, w_layer, z_seq, c_prev_seq, h_seq)
        return dx_seq, (dw_layer, db_layer)

    dx_seq, (dw_all, db_all) = lax.scan(backward_layer, jnp.swapaxes(dy_blk, 0, 1), (weights,) + stored, reverse=True)
    return jnp.swapaxes(dx_seq, 0, 1), dw_all, db_all


def reference(x_in, d_out, weights, biases):
    x_blocks = x_in.reshape(NUM_BLOCKS, BLOCK_ROWS, SEQ, HIDDEN)
    dy_blocks = d_out.reshape(NUM_BLOCKS, BLOCK_ROWS, SEQ, HIDDEN)

    def block_body(grad_acc, block_in):
        dx_blk, dw_all, db_all = block_grads(block_in[0], block_in[1], weights, biases)
        return (grad_acc[0] + dw_all, grad_acc[1] + db_all), dx_blk

    init_acc = (jnp.zeros((LAYERS, 2 * HIDDEN, 4 * HIDDEN), jnp.float32), jnp.zeros((LAYERS, 4 * HIDDEN), jnp.float32))
    (dw_total, db_total), dx_blocks = lax.scan(block_body, init_acc, (x_blocks, dy_blocks))
    return dw_total, db_total, dx_blocks.reshape(BATCH, SEQ, HIDDEN)
```

```python
import functools

import jax
import jax.numpy as jnp
from jax import lax
from jax.experimental import pallas as pl
from jax.experimental.pallas import tpu as pltpu
from jax.sharding import PartitionSpec as P

HID = 512
GATES = 4 * HID
ROWS = 128
OWN = 16
STEPS = 32
PIECE = 4
PIECES = STEPS // PIECE
COL = 256
RING = 4
F32 = jnp.float32
BF16 = jnp.bfloat16
MESH = pl.DeviceIdType.MESH


def dot(a, b):
    return jnp.dot(a, b, preferred_element_type=F32)


def pipeline_kernel(n_data, x_hbm, dout_hbm, w_hbm, b_hbm,
                    dw_hbm, db_ref, dx_hbm, gates_hbm,
                    w, wt, bias, x_buf, h_buf, c_buf, dy_buf, dw_acc, db_acc, xh_t, dz, dr, dc, y_out, g_out, g_in, dx_out,
                    x_sem, xin_sem, xin_send, y_send, g_wsem, g_rsem, dy_sem, din_sem, din_send, dx_send, dxs_send, dx_recv,
                    load_sem):
    layer = lax.axis_index('rep') * n_data + lax.axis_index('data')
    first, last = layer == 0, layer == 7

    def place(idx):
        return {'rep': idx // n_data, 'data': lax.rem(idx, n_data)}

    my_rows = pl.ds(pl.multiple_of(layer * OWN, OWN), OWN)

    w_copy = pltpu.make_async_copy(w_hbm.at[layer], w, load_sem.at[0])
    b_copy = pltpu.make_async_copy(b_hbm.at[layer], bias, load_sem.at[1])
    w_copy.start()
    b_copy.start()

    def x_piece(p, remote):
        src, dst = x_hbm.at[pl.ds(p * PIECE, PIECE)], x_buf.at[pl.ds(p * PIECE, PIECE), my_rows]
        if remote:
            return pltpu.make_async_remote_copy(src, dst, xin_send.at[p], xin_sem.at[p], device_id=place(0), device_id_type=MESH)
        return pltpu.make_async_copy(src, dst, xin_sem.at[p])

    def d_piece(p, remote):
        src, dst = dout_hbm.at[pl.ds(p * PIECE, PIECE)], dy_buf.at[pl.ds(p * PIECE, PIECE), my_rows]
        if remote:
            return pltpu.make_async_remote_copy(src, dst, din_send.at[p], din_sem.at[p], device_id=place(7), device_id_type=MESH)
        return pltpu.make_async_copy(src, dst, din_sem.at[p])

    @pl.when(first)
    def _():
        for p in range(PIECES):
            x_piece(p, False).start()

    @pl.when(jnp.logical_not(first))
    def _():
        for p in range(PIECES):
            x_piece(p, True).start()

    @pl.when(last)
    def _():
        for p in range(PIECES):
            d_piece(p, False).start()

    @pl.when(jnp.logical_not(last))
    def _():
        for p in reversed(range(PIECES // 2, PIECES)):
            d_piece(p, True).start()

    h_buf[0] = jnp.zeros((ROWS, HID), BF16)
    c_buf[0] = jnp.zeros((ROWS, HID), F32)
    w_copy.wait()
    b_copy.wait()

    def make_wt():
        for r in range(4):
            def body(n, carry):
                col = pl.multiple_of(n * COL, COL)
                wt[pl.ds(col, COL), r * COL:(r + 1) * COL] = w[r * COL:(r + 1) * COL, pl.ds(col, COL)].T
                return carry
            lax.fori_loop(0, GATES // COL, body, 0)

    @pl.when(jnp.logical_not(first))
    def _():
        make_wt()

    def y_copy(t, slot):
        return pltpu.make_async_remote_copy(y_out.at[slot], x_buf.at[t], y_send.at[slot], x_sem.at[t],
                                            device_id=place(lax.min(layer + 1, 7)), device_id_type=MESH)

    def g_write(t, slot):
        return pltpu.make_async_copy(g_out.at[slot], gates_hbm.at[t], g_wsem.at[slot])

    def fwd_step(t, carry):
        slot = lax.rem(t, RING)
        gslot = lax.rem(t, 2)

        @pl.when(jnp.logical_and(first, lax.rem(t, PIECE) == 0))
        def _():
            p = t // PIECE
            pltpu.make_async_copy(x_buf.at[pl.ds(p * PIECE, PIECE)], x_buf.at[pl.ds(p * PIECE, PIECE)], xin_sem.at[p]).wait()

        @pl.when(jnp.logical_not(first))
        def _():
            y_copy(t, slot).wait_recv()

        @pl.when(t >= 2)
        def _():
            g_write(t - 2, gslot).wait()

        @pl.when(jnp.logical_and(jnp.logical_not(last), t >= RING))
        def _():
            y_copy(t - RING, slot).wait_send()

        for j in range(HID // COL):
            hc = slice(j * COL, (j + 1) * COL)
            z = []
            for q in range(4):
                cols = slice(q * HID + j * COL, q * HID + (j + 1) * COL)
                z.append(dot(x_buf[t], w[:HID, cols]) + dot(h_buf[t], w[HID:, cols]) + bias[:, cols])
            in_g, fg_g, cand_g, out_g = jax.nn.sigmoid(z[0]), jax.nn.sigmoid(z[1]), jnp.tanh(z[2]), jax.nn.sigmoid(z[3])
            for q, gate in enumerate((in_g, fg_g, cand_g, out_g)):
                g_out[gslot, :, q * HID + j * COL:q * HID + (j + 1) * COL] = gate
            c_new = fg_g * c_buf[t, :, hc] + in_g * cand_g
            h_new = out_g * jnp.tanh(c_new)
            c_buf[t + 1, :, hc] = c_new
            h_buf[t + 1, :, hc] = h_new.astype(BF16)
            y_out[slot, :, hc] = (h_new + x_buf[t, :, hc].astype(F32)).astype(BF16)

        g_write(t, gslot).start()

        @pl.when(jnp.logical_not(last))
        def _():
            y_copy(t, slot).start()
        return carry

    lax.fori_loop(0, STEPS, fwd_step, 0)

    @pl.when(jnp.logical_not(last))
    def _():
        for p in reversed(range(PIECES // 2)):
            d_piece(p, True).start()

    @pl.when(first)
    def _():
        make_wt()

    g_write(STEPS - 2, 0).wait()
    g_write(STEPS - 1, 1).wait()

    def g_read(t, slot):
        return pltpu.make_async_copy(gates_hbm.at[t], g_in.at[slot], g_rsem.at[slot])

    def dy_copy(t, slot):
        return pltpu.make_async_remote_copy(dx_out.at[slot], dy_buf.at[t], dx_send.at[slot], dy_sem.at[t],
                                            device_id=place(lax.max(layer - 1, 0)), device_id_type=MESH)

    def home_copy(t, slot, dev):
        return pltpu.make_async_remote_copy(dx_out.at[slot, dev * OWN:(dev + 1) * OWN], dx_hbm.at[t], dxs_send.at[slot, dev], dx_recv.at[t],
                                            device_id=place(dev), device_id_type=MESH)

    def own_copy(t, slot):
        return pltpu.make_async_copy(dx_out.at[slot, :OWN], dx_hbm.at[t], dxs_send.at[slot, 0])

    g_read(STEPS - 1, 1).start()
    g_read(STEPS - 2, 0).start()
    dr[...] = jnp.zeros((ROWS, HID), F32)
    dc[...] = jnp.zeros((ROWS, HID), F32)
    db_acc[...] = jnp.zeros((8, GATES), F32)
    dw_acc[...] = jnp.zeros((2 * HID, GATES), F32)

    def bwd_step(t, half):
        slot = lax.rem(t, RING)

        @pl.when(jnp.logical_and(last, lax.rem(t, PIECE) == PIECE - 1))
        def _():
            p = t // PIECE
            pltpu.make_async_copy(dy_buf.at[pl.ds(p * PIECE, PIECE)], dy_buf.at[pl.ds(p * PIECE, PIECE)], din_sem.at[p]).wait()

        @pl.when(jnp.logical_not(last))
        def _():
            dy_copy(t, slot).wait_recv()

        g_read(t, half).wait()

        for j in range(HID // COL):
            hc = slice(j * COL, (j + 1) * COL)
            in_g, fg_g, cand_g, out_g = (g_in[half, :, q * HID + j * COL:q * HID + (j + 1) * COL] for q in range(4))
            tanh_c = jnp.tanh(c_buf[t + 1, :, hc])
            dh_tot = dy_buf[t, :, hc] + dr[:, hc]
            dc_tot = dc[:, hc] + dh_tot * out_g * (1.0 - tanh_c * tanh_c)
            parts = (dc_tot * cand_g * in_g * (1.0 - in_g),
                     dc_tot * c_buf[t, :, hc] * fg_g * (1.0 - fg_g),
                     dc_tot * in_g * (1.0 - cand_g * cand_g),
                     dh_tot * tanh_c * out_g * (1.0 - out_g))
            dc[:, hc] = dc_tot * fg_g
            for q, part in enumerate(parts):
                cols = slice(q * HID + j * COL, q * HID + (j + 1) * COL)
                dz[half, :, cols] = part.astype(BF16)
                db_acc[:, cols] += jnp.sum(part.reshape(ROWS // 8, 8, COL), axis=0)

        @pl.when(t >= 2)
        def _():
            g_read(t - 2, half).start()

        @pl.when(jnp.logical_and(jnp.logical_not(first), t < STEPS - RING))
        def _():
            dy_copy(t + RING, slot).wait_send()

        @pl.when(jnp.logical_and(first, t < STEPS - RING))
        def _():
            own_copy(t + RING, slot).wait()
            for dev in range(1, 8):
                home_copy(t + RING, slot, dev).wait_send()

        dr[...] = dot(dz[half], wt[:, HID:])
        dx_out[slot] = dy_buf[t] + dot(dz[half], wt[:, :HID])

        @pl.when(jnp.logical_not(first))
        def _():
            dy_copy(t, slot).start()

        @pl.when(first)
        def _():
            own_copy(t, slot).start()
            for dev in range(1, 8):
                home_copy(t, slot, dev).start()

    def bwd_pair(k, carry):
        t0 = STEPS - 2 - 2 * k
        xh_t[:HID] = x_buf[pl.ds(t0, 2)].reshape(2 * ROWS, HID).T
        xh_t[HID:] = h_buf[pl.ds(t0, 2)].reshape(2 * ROWS, HID).T
        bwd_step(t0 + 1, 1)
        bwd_step(t0, 0)
        def block(n, c):
            cols = pl.ds(pl.multiple_of(n * COL, COL), COL)
            dw_acc[:, cols] += dot(xh_t[...], dz[:, :, cols].reshape(2 * ROWS, COL))
            return c
        lax.fori_loop(0, GATES // COL, block, 0)
        return carry

    lax.fori_loop(0, STEPS // 2, bwd_pair, 0)

    dw_copy = pltpu.make_async_copy(dw_acc, dw_hbm.at[0], load_sem.at[0])
    dw_copy.start()
    db_ref[...] = jnp.sum(db_acc[...], axis=0, keepdims=True)

    @pl.when(jnp.logical_not(last))
    def _():
        for s in range(RING):
            y_copy(STEPS - RING + s, s).wait_send()
        for p in range(PIECES):
            d_piece(p, True).wait_send()

    @pl.when(jnp.logical_not(first))
    def _():
        for s in range(RING):
            dy_copy(s, s).wait_send()
        for p in range(PIECES):
            x_piece(p, True).wait_send()
        for t in range(STEPS):
            home_copy(t, 0, 0).wait_recv()

    @pl.when(first)
    def _():
        for s in range(RING):
            own_copy(s, s).wait()
            for dev in range(1, 8):
                home_copy(s, s, dev).wait_send()

    dw_copy.wait()


def solution(mesh):
    batch_axes = tuple(mesh.axis_names)
    n_data = mesh.shape['data']

    def device_step(x_in, d_out, weights, biases):
        x_seq = jnp.swapaxes(x_in, 0, 1)
        d_seq = jnp.swapaxes(d_out, 0, 1)
        hbm = pl.BlockSpec(memory_space=pl.ANY)
        dma = pltpu.SemaphoreType.DMA
        dw, db, dx, _ = pl.pallas_call(
            functools.partial(pipeline_kernel, n_data),
            out_shape=(jax.ShapeDtypeStruct((1, 2 * HID, GATES), F32),
                       jax.ShapeDtypeStruct((1, GATES), F32),
                       jax.ShapeDtypeStruct((STEPS, OWN, HID), F32),
                       jax.ShapeDtypeStruct((STEPS, ROWS, GATES), F32)),
            in_specs=[hbm] * 4,
            out_specs=(hbm, pl.BlockSpec(memory_space=pltpu.VMEM), hbm, hbm),
            scratch_shapes=[
                pltpu.VMEM((2 * HID, GATES), BF16),
                pltpu.VMEM((GATES, 2 * HID), BF16),
                pltpu.VMEM((1, GATES), F32),
                pltpu.VMEM((STEPS, ROWS, HID), BF16),
                pltpu.VMEM((STEPS + 1, ROWS, HID), BF16),
                pltpu.VMEM((STEPS + 1, ROWS, HID), F32),
                pltpu.VMEM((STEPS, ROWS, HID), F32),
                pltpu.VMEM((2 * HID, GATES), F32),
                pltpu.VMEM((8, GATES), F32),
                pltpu.VMEM((2 * HID, 2 * ROWS), BF16),
                pltpu.VMEM((2, ROWS, GATES), BF16),
                pltpu.VMEM((ROWS, HID), F32),
                pltpu.VMEM((ROWS, HID), F32),
                pltpu.VMEM((RING, ROWS, HID), BF16),
                pltpu.VMEM((2, ROWS, GATES), F32),
                pltpu.VMEM((2, ROWS, GATES), F32),
                pltpu.VMEM((RING, ROWS, HID), F32),
                dma((STEPS,)), dma((PIECES,)), dma((PIECES,)), dma((RING,)), dma((2,)), dma((2,)),
                dma((STEPS,)), dma((PIECES,)), dma((PIECES,)), dma((RING,)), dma((RING, 8)), dma((STEPS,)),
                dma((2,)),
            ],
            compiler_params=pltpu.CompilerParams(has_side_effects=True, vmem_limit_bytes=66000000),
        )(x_seq, d_seq, weights, biases.reshape(8, 1, GATES))
        dw_all = lax.all_gather(dw, batch_axes, axis=0, tiled=True)
        db_all = lax.all_gather(db, batch_axes, axis=0, tiled=True)
        return dw_all, db_all, jnp.swapaxes(dx, 0, 1)

    return jax.shard_map(device_step, mesh=mesh,
                         in_specs=(P(batch_axes), P(batch_axes), P(), P()),
                         out_specs=(P(), P(), P(batch_axes)), check_vma=False)
```

```python
import functools

import jax
import jax.numpy as jnp
from jax import lax
from jax.experimental import pallas as pl
from jax.experimental.pallas import tpu as pltpu
from jax.sharding import PartitionSpec as P

HID = 512
GATES = 4 * HID
ROWS = 128
OWN = 16
STEPS = 32
LOCAL = 4
CHIPS = 4
PIECE = 4
PIECES = STEPS // PIECE
COL = 256
KT = 2 * HID // COL
NT = GATES // COL
REC = 5 * HID
RING = 4
F32 = jnp.float32
BF16 = jnp.bfloat16
MESH = pl.DeviceIdType.MESH


def dot(a, b):
    return jnp.dot(a, b, preferred_element_type=F32)


def sum_dots(pairs):
    total = None
    for a, b in pairs:
        part = dot(a, b)
        total = part if total is None else total + part
    return total


def recurrence_kernel(n_data, x_hbm, dout_hbm, w_hbm, bias,
                      xh_hbm, dz_hbm, dx_hbm, db_hbm, rec_hbm,
                      w, x_buf, dy_buf, lhs, hn, xn, cs, rec, y_out, dz, dyn, dr, dc, dx_out, db_acc, db_sum,
                      w_sem, x_sem, xin_sem, xin_send, y_send, lhs_sem, rec_wsem, rec_rsem, dy_sem, din_sem, din_send,
                      dz_sem, dx_send, home_sem, dx_recv, db_sem):
    rep, data = lax.axis_index('rep'), lax.axis_index('data')
    core = lax.rem(data, 2)
    chip = rep * (n_data // 2) + data // 2
    me = 2 * chip + core
    first, second = core == 0, core == 1
    partner = {'rep': rep, 'data': data + 1 - 2 * core}
    my_rows = pl.ds(pl.multiple_of(me * OWN, OWN), OWN)

    def place(dev):
        return {'rep': dev // n_data, 'data': dev % n_data}

    def w_copy(l, k, n):
        return pltpu.make_async_copy(w_hbm.at[core * LOCAL + l, pl.ds(k * COL, COL), pl.ds(n * COL, COL)], w.at[l, k, n], w_sem.at[l])

    def x_piece(p, dev, remote):
        src, dst = x_hbm.at[pl.ds(p * PIECE, PIECE)], x_buf.at[pl.ds(p * PIECE, PIECE), my_rows]
        if remote:
            return pltpu.make_async_remote_copy(src, dst, xin_send.at[p, dev // 2], xin_sem.at[p], device_id=place(dev), device_id_type=MESH)
        return pltpu.make_async_copy(src, dst, xin_sem.at[p])

    def d_piece(p, dev, remote):
        src, dst = dout_hbm.at[pl.ds(p * PIECE, PIECE)], dy_buf.at[pl.ds(p * PIECE, PIECE), my_rows]
        if remote:
            return pltpu.make_async_remote_copy(src, dst, din_send.at[p, dev // 2], din_sem.at[p], device_id=place(dev), device_id_type=MESH)
        return pltpu.make_async_copy(src, dst, din_sem.at[p])

    def gather(piece, p, which):
        for dev in range(which, 2 * CHIPS, 2):
            @pl.when(me == dev)
            def _():
                piece(p, dev, False).start()

            @pl.when(me != dev)
            def _():
                piece(p, dev, True).start()

    def gathered(piece, p, which):
        for dev in range(which, 2 * CHIPS, 2):
            @pl.when(me != dev)
            def _():
                piece(p, dev, True).wait_send()

    for p in range(PIECES):
        gather(x_piece, p, 0)
    for l in range(LOCAL):
        for k in range(KT):
            for n in range(NT):
                w_copy(l, k, n).start()
    for p in reversed(range(PIECES)):
        gather(d_piece, p, 1)

    for l in range(LOCAL):
        hn[l][...] = jnp.zeros((ROWS, HID), BF16)
        cs[l][...] = jnp.zeros((ROWS, HID), F32)
    for l in range(LOCAL):
        for k in range(KT):
            for n in range(NT):
                w_copy(l, k, n).wait()

    def y_copy(t, slot):
        return pltpu.make_async_remote_copy(y_out.at[slot], x_buf.at[t], y_send.at[slot], x_sem.at[t], device_id=partner, device_id_type=MESH)

    def lhs_write(l, t, slot):
        return pltpu.make_async_copy(lhs[l].at[slot], xh_hbm.at[l, t], lhs_sem.at[l, slot])

    def rec_write(l, t, slot):
        return pltpu.make_async_copy(rec[l].at[slot], rec_hbm.at[l, t], rec_wsem.at[l, slot])

    def guard(cond):
        if isinstance(cond, bool):
            return (lambda f: f()) if cond else (lambda f: None)
        return pl.when(cond)

    def valid(t, full):
        return True if full else jnp.logical_and(t >= 0, t < STEPS)

    def both(a, b):
        return b if a is True else jnp.logical_and(a, b)

    def fwd_cell(l, t, slot):
        for j in range(HID // COL):
            hc = slice(j * COL, (j + 1) * COL)
            z = []
            for q in range(4):
                n = q * (HID // COL) + j
                z.append(sum_dots([(lhs[l][slot, :, k * COL:(k + 1) * COL], w[l, k, n]) for k in range(KT)])
                         + bias[pl.ds(core * LOCAL + l, 1), n * COL:(n + 1) * COL])
            in_g, fg_g, cand_g, out_g = jax.nn.sigmoid(z[0]), jax.nn.sigmoid(z[1]), jnp.tanh(z[2]), jax.nn.sigmoid(z[3])
            c_prev = cs[l][:, hc]
            for q, value in enumerate((in_g, fg_g, cand_g, out_g, c_prev)):
                rec[l][slot, :, q * HID + j * COL:q * HID + (j + 1) * COL] = value
            c_new = fg_g * c_prev + in_g * cand_g
            h_new = out_g * jnp.tanh(c_new)
            cs[l][:, hc] = c_new
            hn[l][:, hc] = h_new.astype(BF16)
            y_new = (h_new + lhs[l][slot, :, hc].astype(F32)).astype(BF16)
            if l < LOCAL - 1:
                xn[l][:, hc] = y_new
            else:
                y_out[lax.rem(t, RING), :, hc] = y_new

    def fwd_wave(s, full):
        t_of = [s - l for l in range(LOCAL)]
        slot_of = [lax.rem(t + RING, 2) for t in t_of]

        @pl.when(jnp.logical_and(first, both(valid(s, full), lax.rem(s, PIECE) == 0)))
        def _():
            p = s // PIECE
            pltpu.make_async_copy(x_buf.at[pl.ds(p * PIECE, PIECE)], x_buf.at[pl.ds(p * PIECE, PIECE)], xin_sem.at[p]).wait()

        @pl.when(both(valid(s, full), second))
        def _():
            y_copy(s, 0).wait_recv()

        for l in range(LOCAL):
            t, slot = t_of[l], slot_of[l]

            @guard(True if full else jnp.logical_and(t >= 2, t < STEPS))
            def _():
                lhs_write(l, t - 2, slot).wait()
                rec_write(l, t - 2, slot).wait()

        t_top = t_of[LOCAL - 1]

        @pl.when(jnp.logical_and(first, jnp.logical_and(t_top >= RING, t_top < STEPS)))
        def _():
            y_copy(t_top - RING, lax.rem(t_top, RING)).wait_send()

        def assemble(l):
            lhs[l][slot_of[l], :, :HID] = x_buf[t_of[0]] if l == 0 else xn[l - 1][...]
            lhs[l][slot_of[l], :, HID:] = hn[l][...]

        if full:
            for l in range(LOCAL):
                assemble(l)
            for l in range(LOCAL):
                fwd_cell(l, t_of[l], slot_of[l])
        else:
            for l in reversed(range(LOCAL)):
                @pl.when(valid(t_of[l], False))
                def _():
                    assemble(l)
                    fwd_cell(l, t_of[l], slot_of[l])

        for l in range(LOCAL):
            t, slot = t_of[l], slot_of[l]

            @guard(valid(t, full))
            def _():
                lhs_write(l, t, slot).start()

            @pl.when(both(valid(t, full), t < STEPS - 2))
            def _():
                rec_write(l, t, slot).start()

        @pl.when(both(valid(t_top, full), first))
        def _():
            y_copy(t_top, lax.rem(t_top, RING)).start()

    def run_waves(wave, lo, hi, full):
        def body(s, carry):
            wave(s, full)
            return carry
        lax.fori_loop(lo, hi, body, 0)

    run_waves(fwd_wave, 0, LOCAL + 1, False)
    run_waves(fwd_wave, LOCAL + 1, STEPS, True)
    run_waves(fwd_wave, STEPS, STEPS + LOCAL - 1, False)

    def turn(i, carry):
        k, n = i // NT, lax.rem(i, NT)
        for l0 in range(0, LOCAL, 2):
            tiles = [w[l, k, n].T for l in (l0, l0 + 1)]
            for l, tile in zip((l0, l0 + 1), tiles):
                w[l, k, n] = tile
        return carry

    lax.fori_loop(0, KT * NT, turn, 0)

    for l in range(LOCAL):
        for slot in range(2):
            lhs_write(l, STEPS - 2 + slot, slot).wait()

    def rec_read(l, t, slot):
        return pltpu.make_async_copy(rec_hbm.at[l, t], rec[l].at[slot], rec_rsem.at[l, slot])

    def dz_write(l, t, slot):
        return pltpu.make_async_copy(dz[l].at[slot], dz_hbm.at[l, t], dz_sem.at[l, slot])

    def dy_copy(t, slot):
        return pltpu.make_async_remote_copy(dx_out.at[slot], dy_buf.at[t], dx_send.at[slot], dy_sem.at[t], device_id=partner, device_id_type=MESH)

    def home_copy(t, slot):
        rows = pl.ds(pl.multiple_of((2 * chip + 1) * OWN, OWN), OWN)
        return pltpu.make_async_remote_copy(dx_out.at[slot, rows], dx_hbm.at[t], dx_send.at[slot], dx_recv.at[t], device_id=partner, device_id_type=MESH)

    def own_copy(t, slot):
        return pltpu.make_async_copy(dx_out.at[slot, my_rows], dx_hbm.at[t], home_sem.at[slot])

    for l in range(LOCAL):
        dr[l][...] = jnp.zeros((ROWS, HID), F32)
        dc[l][...] = jnp.zeros((ROWS, HID), F32)
    db_acc[...] = jnp.zeros((LOCAL, 8, GATES), F32)

    def bwd_cell(l, t, slot):
        out_slot = lax.rem(t, RING)
        for j in range(HID // COL):
            hc = slice(j * COL, (j + 1) * COL)
            in_g, fg_g, cand_g, out_g, c_prev = (rec[l][slot, :, q * HID + j * COL:q * HID + (j + 1) * COL] for q in range(5))
            tanh_c = jnp.tanh(fg_g * c_prev + in_g * cand_g)
            dy = dy_buf[t, :, hc] if l == LOCAL - 1 else dyn[l][:, hc]
            dh_tot = dy + dr[l][:, hc]
            dc_tot = dc[l][:, hc] + dh_tot * out_g * (1.0 - tanh_c * tanh_c)
            parts = (dc_tot * cand_g * in_g * (1.0 - in_g),
                     dc_tot * c_prev * fg_g * (1.0 - fg_g),
                     dc_tot * in_g * (1.0 - cand_g * cand_g),
                     dh_tot * tanh_c * out_g * (1.0 - out_g))
            dc[l][:, hc] = dc_tot * fg_g
            for q, part in enumerate(parts):
                cols = slice(q * HID + j * COL, q * HID + (j + 1) * COL)
                dz[l][slot, :, cols] = part.astype(BF16)
                db_acc[l, :, cols] += jnp.sum(part.reshape(ROWS // 8, 8, COL), axis=0)
        for k in range(KT):
            prod = sum_dots([(dz[l][slot, :, n * COL:(n + 1) * COL], w[l, k, n]) for n in range(NT)])
            if k >= KT // 2:
                dr[l][:, (k - KT // 2) * COL:(k - KT // 2 + 1) * COL] = prod
            else:
                kc = slice(k * COL, (k + 1) * COL)
                total = (dy_buf[t, :, kc] if l == LOCAL - 1 else dyn[l][:, kc]) + prod
                if l > 0:
                    dyn[l - 1][:, kc] = total
                else:
                    dx_out[out_slot, :, kc] = total

    def bwd_wave(s, full):
        t_of = [STEPS + LOCAL - 2 - s - l for l in range(LOCAL)]
        slot_of = [lax.rem(t + RING, 2) for t in t_of]
        t_top, t_low = t_of[LOCAL - 1], t_of[0]
        out_slot = lax.rem(t_low + 2 * RING, RING)

        @pl.when(jnp.logical_and(second, both(valid(t_top, full), lax.rem(t_top, PIECE) == PIECE - 1)))
        def _():
            p = t_top // PIECE
            pltpu.make_async_copy(dy_buf.at[pl.ds(p * PIECE, PIECE)], dy_buf.at[pl.ds(p * PIECE, PIECE)], din_sem.at[p]).wait()

        @pl.when(both(valid(t_top, full), first))
        def _():
            dy_copy(t_top, 0).wait_recv()

        for l in range(LOCAL):
            t, slot = t_of[l], slot_of[l]

            @guard(True if full else jnp.logical_and(t >= 0, t < STEPS - 2))
            def _():
                rec_read(l, t, slot).wait()
                dz_write(l, t + 2, slot).wait()

        @pl.when(jnp.logical_and(t_low >= 0, t_low < STEPS - RING))
        def _():
            @pl.when(second)
            def _():
                dy_copy(t_low + RING, out_slot).wait_send()

            @pl.when(first)
            def _():
                home_copy(t_low + RING, out_slot).wait_send()
                own_copy(t_low + RING, out_slot).wait()

        for l in range(LOCAL):
            if full:
                bwd_cell(l, t_of[l], slot_of[l])
            else:
                @pl.when(valid(t_of[l], False))
                def _():
                    bwd_cell(l, t_of[l], slot_of[l])

        for l in range(LOCAL):
            t, slot = t_of[l], slot_of[l]

            @pl.when(both(valid(t, full), t >= 2))
            def _():
                rec_read(l, t - 2, slot).start()

            @guard(valid(t, full))
            def _():
                dz_write(l, t, slot).start()

        @pl.when(both(valid(t_low, full), second))
        def _():
            dy_copy(t_low, out_slot).start()

        @pl.when(both(valid(t_low, full), first))
        def _():
            home_copy(t_low, out_slot).start()
            own_copy(t_low, out_slot).start()

    run_waves(bwd_wave, 0, LOCAL + 1, False)
    run_waves(bwd_wave, LOCAL + 1, STEPS, True)
    run_waves(bwd_wave, STEPS, STEPS + LOCAL - 1, False)

    for l in range(LOCAL):
        db_sum[l:l + 1, :] = jnp.sum(db_acc[l], axis=0, keepdims=True)
    db_local = pltpu.make_async_copy(db_sum, db_hbm.at[core], db_sem.at[0])
    db_remote = pltpu.make_async_remote_copy(db_sum, db_hbm.at[core], db_sem.at[1], db_sem.at[2], device_id=partner, device_id_type=MESH)
    db_local.start()
    db_remote.start()

    for p in range(PIECES):
        gathered(x_piece, p, 0)
        gathered(d_piece, p, 1)
    for l in range(LOCAL):
        for slot in range(2):
            dz_write(l, slot, slot).wait()

    @pl.when(first)
    def _():
        for s in range(RING):
            y_copy(STEPS - RING + s, s).wait_send()
            home_copy(s, s).wait_send()
            own_copy(s, s).wait()

    @pl.when(second)
    def _():
        for s in range(RING):
            dy_copy(s, s).wait_send()
        for t in range(STEPS):
            home_copy(t, 0).wait_recv()

    db_local.wait()
    db_remote.wait()


def recurrence_entry(n_data, *refs):
    ins, outs, rest = refs[:4], refs[4:9], list(refs[9:])
    take = lambda count: [rest.pop(0) for _ in range(count)]
    w, x_buf, dy_buf = take(3)
    lhs, hn, xn, cs, rec = take(4), take(4), take(3), take(4), take(4)
    y_out, = take(1)
    dz, dyn, dr, dc = take(4), take(3), take(4), take(4)
    dx_out, db_acc, db_sum = take(3)
    recurrence_kernel(n_data, *ins, *outs, w, x_buf, dy_buf, lhs, hn, xn, cs, rec, y_out, dz, dyn, dr, dc, dx_out, db_acc, db_sum, *rest)


def weight_kernel(n_data, xh, dz, dw_hbm, stage, local_sem, send_sem, recv_sem):
    rep, data = lax.axis_index('rep'), lax.axis_index('data')
    core = lax.rem(data, 2)
    partner = {'rep': rep, 'data': data + 1 - 2 * core}
    i = pl.program_id(0)
    total = LOCAL * NT
    slot = lax.rem(i, 2)

    def out(step):
        return dw_hbm.at[core * LOCAL + step // NT, :, pl.ds(pl.multiple_of(lax.rem(step, NT) * COL, COL), COL)]

    def near(step, slot):
        return pltpu.make_async_copy(stage.at[slot], out(step), local_sem.at[slot])

    def far(step, slot):
        return pltpu.make_async_remote_copy(stage.at[slot], out(step), send_sem.at[slot], recv_sem.at[step], device_id=partner, device_id_type=MESH)

    @pl.when(i >= 2)
    def _():
        near(i - 2, slot).wait()
        far(i - 2, slot).wait_send()

    stage[slot] = lax.dot_general(xh[0], dz[0], (((0,), (0,)), ((), ())), preferred_element_type=F32)
    near(i, slot).start()
    far(i, slot).start()

    @pl.when(i == total - 1)
    def _():
        for back in range(2):
            near(total - 2 + back, back).wait()
            far(total - 2 + back, back).wait_send()
        for step in range(total):
            far(step, 0).wait_recv()


def solution(mesh):
    batch_axes = tuple(mesh.axis_names)
    n_data = mesh.shape['data']
    hbm = pl.BlockSpec(memory_space=pl.ANY)
    dma = pltpu.SemaphoreType.DMA

    def device_step(x_in, d_out, weights, biases):
        x_seq = jnp.swapaxes(x_in, 0, 1)
        d_seq = jnp.swapaxes(d_out, 0, 1)
        plane = lambda dtype: pltpu.VMEM((ROWS, HID), dtype)
        xh, dz, dx, db, _ = pl.pallas_call(
            functools.partial(recurrence_entry, n_data),
            out_shape=(jax.ShapeDtypeStruct((LOCAL, STEPS, ROWS, 2 * HID), BF16),
                       jax.ShapeDtypeStruct((LOCAL, STEPS, ROWS, GATES), BF16),
                       jax.ShapeDtypeStruct((STEPS, OWN, HID), F32),
                       jax.ShapeDtypeStruct((2, LOCAL, GATES), F32),
                       jax.ShapeDtypeStruct((LOCAL, STEPS, ROWS, REC), F32)),
            in_specs=[hbm, hbm, hbm, pl.BlockSpec(memory_space=pltpu.VMEM)],
            out_specs=(hbm,) * 5,
            scratch_shapes=[
                pltpu.VMEM((LOCAL, KT, NT, COL, COL), BF16),
                pltpu.VMEM((STEPS, ROWS, HID), BF16),
                pltpu.VMEM((STEPS, ROWS, HID), F32),
                *[pltpu.VMEM((2, ROWS, 2 * HID), BF16)] * 4,
                *[plane(BF16)] * 4,
                *[plane(BF16)] * 3,
                *[plane(F32)] * 4,
                *[pltpu.VMEM((2, ROWS, REC), F32)] * 4,
                pltpu.VMEM((RING, ROWS, HID), BF16),
                *[pltpu.VMEM((2, ROWS, GATES), BF16)] * 4,
                *[plane(F32)] * 3,
                *[plane(F32)] * 4,
                *[plane(F32)] * 4,
                pltpu.VMEM((RING, ROWS, HID), F32),
                pltpu.VMEM((LOCAL, 8, GATES), F32),
                pltpu.VMEM((LOCAL, GATES), F32),
                dma((LOCAL,)), dma((STEPS,)), dma((PIECES,)), dma((PIECES, CHIPS)), dma((RING,)), dma((LOCAL, 2)), dma((LOCAL, 2)), dma((LOCAL, 2)),
                dma((STEPS,)), dma((PIECES,)), dma((PIECES, CHIPS)), dma((LOCAL, 2)), dma((RING,)), dma((RING,)), dma((STEPS,)), dma((3,)),
            ],
            compiler_params=pltpu.CompilerParams(has_side_effects=True, vmem_limit_bytes=66000000),
        )(x_seq, d_seq, weights, biases)
        dw = pl.pallas_call(
            functools.partial(weight_kernel, n_data),
            out_shape=jax.ShapeDtypeStruct((2 * LOCAL, 2 * HID, GATES), F32),
            grid=(LOCAL * NT,),
            in_specs=[pl.BlockSpec((1, STEPS * ROWS, 2 * HID), lambda i: (i // NT, 0, 0)),
                      pl.BlockSpec((1, STEPS * ROWS, COL), lambda i: (i // NT, 0, lax.rem(i, NT)))],
            out_specs=hbm,
            scratch_shapes=[pltpu.VMEM((2, 2 * HID, COL), F32), dma((2,)), dma((2,)), dma((LOCAL * NT,))],
            compiler_params=pltpu.CompilerParams(has_side_effects=True, vmem_limit_bytes=60000000),
        )(xh.reshape(LOCAL, STEPS * ROWS, 2 * HID), dz.reshape(LOCAL, STEPS * ROWS, GATES))
        return dw, db.reshape(2 * LOCAL, GATES), jnp.swapaxes(dx, 0, 1)

    return jax.shard_map(device_step, mesh=mesh,
                         in_specs=(P(batch_axes), P(batch_axes), P(), P()),
                         out_specs=(P(), P(), P(batch_axes)), check_vma=False)
```

```python
import functools

import jax
import jax.numpy as jnp
from jax import lax
from jax.experimental import pallas as pl
from jax.experimental.pallas import tpu as pltpu
from jax.sharding import PartitionSpec as P

HID = 512
GATES = 4 * HID
ROWS = 128
OWN = 16
STEPS = 32
LOCAL = 4
CHIPS = 4
PIECE = 4
PIECES = STEPS // PIECE
COL = 256
KT = 2 * HID // COL
NT = GATES // COL
REC = 5 * HID
RING = 4
SLOTS = 3
F32 = jnp.float32
BF16 = jnp.bfloat16
MESH = pl.DeviceIdType.MESH


def dot(a, b):
    return jnp.dot(a, b, preferred_element_type=F32)


def sum_dots(pairs):
    total = None
    for a, b in pairs:
        part = dot(a, b)
        total = part if total is None else total + part
    return total


def recurrence_kernel(n_data, x_hbm, dout_hbm, w_hbm, bias,
                      xh_hbm, dz_hbm, dx_hbm, db_hbm, rec_hbm,
                      w, x_buf, dy_buf, lhs, hn, xn, cs, rec, y_out, dz, dyn, dr, dc, dx_out, db_acc, db_sum,
                      w_sem, x_sem, xin_sem, xin_send, y_send, lhs_sem, rec_wsem, rec_rsem, dy_sem, din_sem, din_send,
                      dz_sem, dx_send, home_sem, dx_recv, db_sem):
    rep, data = lax.axis_index('rep'), lax.axis_index('data')
    core = lax.rem(data, 2)
    chip = rep * (n_data // 2) + data // 2
    me = 2 * chip + core
    first, second = core == 0, core == 1
    partner = {'rep': rep, 'data': data + 1 - 2 * core}
    my_rows = pl.ds(pl.multiple_of(me * OWN, OWN), OWN)

    def place(dev):
        return {'rep': dev // n_data, 'data': dev % n_data}

    def w_copy(l, k, n):
        return pltpu.make_async_copy(w_hbm.at[core * LOCAL + l, pl.ds(k * COL, COL), pl.ds(n * COL, COL)], w.at[l, k, n], w_sem.at[l])

    def x_piece(p, dev, remote):
        src, dst = x_hbm.at[pl.ds(p * PIECE, PIECE)], x_buf.at[pl.ds(p * PIECE, PIECE), my_rows]
        if remote:
            return pltpu.make_async_remote_copy(src, dst, xin_send.at[p, dev // 2], xin_sem.at[p], device_id=place(dev), device_id_type=MESH)
        return pltpu.make_async_copy(src, dst, xin_sem.at[p])

    def d_piece(p, dev, remote):
        src, dst = dout_hbm.at[pl.ds(p * PIECE, PIECE)], dy_buf.at[pl.ds(p * PIECE, PIECE), my_rows]
        if remote:
            return pltpu.make_async_remote_copy(src, dst, din_send.at[p, dev // 2], din_sem.at[p], device_id=place(dev), device_id_type=MESH)
        return pltpu.make_async_copy(src, dst, din_sem.at[p])

    def gather(piece, p, which):
        for dev in range(which, 2 * CHIPS, 2):
            @pl.when(me == dev)
            def _():
                piece(p, dev, False).start()

            @pl.when(me != dev)
            def _():
                piece(p, dev, True).start()

    def gathered(piece, p, which):
        for dev in range(which, 2 * CHIPS, 2):
            @pl.when(me != dev)
            def _():
                piece(p, dev, True).wait_send()

    for p in range(PIECES):
        gather(x_piece, p, 0)
    for l in range(LOCAL):
        for k in range(KT):
            for n in range(NT):
                w_copy(l, k, n).start()
    for p in reversed(range(PIECES)):
        gather(d_piece, p, 1)

    for l in range(LOCAL):
        hn[l][...] = jnp.zeros((ROWS, HID), BF16)
        cs[l][...] = jnp.zeros((ROWS, HID), F32)
    for l in range(LOCAL):
        for k in range(KT):
            for n in range(NT):
                w_copy(l, k, n).wait()

    def y_copy(t, slot):
        return pltpu.make_async_remote_copy(y_out.at[slot], x_buf.at[t], y_send.at[slot], x_sem.at[t], device_id=partner, device_id_type=MESH)

    def lhs_write(l, t, slot):
        return pltpu.make_async_copy(lhs[l].at[slot], xh_hbm.at[l, t], lhs_sem.at[l, slot])

    def rec_write(l, t, slot):
        return pltpu.make_async_copy(rec[l].at[slot], rec_hbm.at[l, t], rec_wsem.at[l, slot])

    def guard(cond):
        if isinstance(cond, bool):
            return (lambda f: f()) if cond else (lambda f: None)
        return pl.when(cond)

    def valid(t, full):
        return True if full else jnp.logical_and(t >= 0, t < STEPS)

    def both(a, b):
        return b if a is True else jnp.logical_and(a, b)

    def fwd_cell(l, t, slot):
        for j in range(HID // COL):
            hc = slice(j * COL, (j + 1) * COL)
            z = []
            for q in range(4):
                n = q * (HID // COL) + j
                z.append(sum_dots([(lhs[l][slot, :, k * COL:(k + 1) * COL], w[l, k, n]) for k in range(KT)])
                         + bias[pl.ds(core * LOCAL + l, 1), n * COL:(n + 1) * COL])
            in_g, fg_g, cand_g, out_g = jax.nn.sigmoid(z[0]), jax.nn.sigmoid(z[1]), jnp.tanh(z[2]), jax.nn.sigmoid(z[3])
            c_prev = cs[l][:, hc]
            for q, value in enumerate((in_g, fg_g, cand_g, out_g, c_prev)):
                rec[l][slot, :, q * HID + j * COL:q * HID + (j + 1) * COL] = value
            c_new = fg_g * c_prev + in_g * cand_g
            h_new = out_g * jnp.tanh(c_new)
            cs[l][:, hc] = c_new
            hn[l][:, hc] = h_new.astype(BF16)
            y_new = (h_new + lhs[l][slot, :, hc].astype(F32)).astype(BF16)
            if l < LOCAL - 1:
                xn[l][:, hc] = y_new
            else:
                y_out[lax.rem(t, RING), :, hc] = y_new

    def fwd_wave(s, full):
        t_of = [s - l for l in range(LOCAL)]
        slot_of = [lax.rem(t + SLOTS, SLOTS) for t in t_of]

        @pl.when(jnp.logical_and(first, both(valid(s, full), lax.rem(s, PIECE) == 0)))
        def _():
            p = s // PIECE
            pltpu.make_async_copy(x_buf.at[pl.ds(p * PIECE, PIECE)], x_buf.at[pl.ds(p * PIECE, PIECE)], xin_sem.at[p]).wait()

        @pl.when(both(valid(s, full), second))
        def _():
            y_copy(s, 0).wait_recv()

        for l in range(LOCAL):
            t, slot = t_of[l], slot_of[l]

            @guard(True if full else jnp.logical_and(t >= SLOTS, t < STEPS))
            def _():
                lhs_write(l, t - SLOTS, slot).wait()
                rec_write(l, t - SLOTS, slot).wait()

        t_top = t_of[LOCAL - 1]

        @pl.when(jnp.logical_and(first, jnp.logical_and(t_top >= RING, t_top < STEPS)))
        def _():
            y_copy(t_top - RING, lax.rem(t_top, RING)).wait_send()

        def assemble(l):
            lhs[l][slot_of[l], :, :HID] = x_buf[t_of[0]] if l == 0 else xn[l - 1][...]
            lhs[l][slot_of[l], :, HID:] = hn[l][...]

        if full:
            for l in range(LOCAL):
                assemble(l)
            for l in range(LOCAL):
                fwd_cell(l, t_of[l], slot_of[l])
        else:
            for l in reversed(range(LOCAL)):
                @pl.when(valid(t_of[l], False))
                def _():
                    assemble(l)
                    fwd_cell(l, t_of[l], slot_of[l])

        for l in range(LOCAL):
            t, slot = t_of[l], slot_of[l]

            @guard(valid(t, full))
            def _():
                lhs_write(l, t, slot).start()

            @pl.when(both(valid(t, full), t < STEPS - SLOTS))
            def _():
                rec_write(l, t, slot).start()

        @pl.when(both(valid(t_top, full), first))
        def _():
            y_copy(t_top, lax.rem(t_top, RING)).start()

    def run_waves(wave, lo, hi, full):
        def body(s, carry):
            wave(s, full)
            return carry
        lax.fori_loop(lo, hi, body, 0)

    run_waves(fwd_wave, 0, LOCAL - 1 + SLOTS, False)
    run_waves(fwd_wave, LOCAL - 1 + SLOTS, STEPS, True)
    run_waves(fwd_wave, STEPS, STEPS + LOCAL - 1, False)

    def turn(i, carry):
        k, n = i // NT, lax.rem(i, NT)
        for l0 in range(0, LOCAL, 2):
            tiles = [w[l, k, n].T for l in (l0, l0 + 1)]
            for l, tile in zip((l0, l0 + 1), tiles):
                w[l, k, n] = tile
        return carry

    lax.fori_loop(0, KT * NT, turn, 0)

    for l in range(LOCAL):
        for t in range(STEPS - SLOTS, STEPS):
            lhs_write(l, t, t % SLOTS).wait()

    def rec_read(l, t, slot):
        return pltpu.make_async_copy(rec_hbm.at[l, t], rec[l].at[slot], rec_rsem.at[l, slot])

    def dz_write(l, t, slot):
        return pltpu.make_async_copy(dz[l].at[slot], dz_hbm.at[l, t], dz_sem.at[l, slot])

    def dy_copy(t, slot):
        return pltpu.make_async_remote_copy(dx_out.at[slot], dy_buf.at[t], dx_send.at[slot], dy_sem.at[t], device_id=partner, device_id_type=MESH)

    def home_copy(t, slot):
        rows = pl.ds(pl.multiple_of((2 * chip + 1) * OWN, OWN), OWN)
        return pltpu.make_async_remote_copy(dx_out.at[slot, rows], dx_hbm.at[t], dx_send.at[slot], dx_recv.at[t], device_id=partner, device_id_type=MESH)

    def own_copy(t, slot):
        return pltpu.make_async_copy(dx_out.at[slot, my_rows], dx_hbm.at[t], home_sem.at[slot])

    for l in range(LOCAL):
        dr[l][...] = jnp.zeros((ROWS, HID), F32)
        dc[l][...] = jnp.zeros((ROWS, HID), F32)
    db_acc[...] = jnp.zeros((LOCAL, 8, GATES), F32)

    def bwd_cell(l, t, slot):
        out_slot = lax.rem(t, RING)
        for j in range(HID // COL):
            hc = slice(j * COL, (j + 1) * COL)
            in_g, fg_g, cand_g, out_g, c_prev = (rec[l][slot, :, q * HID + j * COL:q * HID + (j + 1) * COL] for q in range(5))
            tanh_c = jnp.tanh(fg_g * c_prev + in_g * cand_g)
            dy = dy_buf[t, :, hc] if l == LOCAL - 1 else dyn[l][:, hc]
            dh_tot = dy + dr[l][:, hc]
            dc_tot = dc[l][:, hc] + dh_tot * out_g * (1.0 - tanh_c * tanh_c)
            parts = (dc_tot * cand_g * in_g * (1.0 - in_g),
                     dc_tot * c_prev * fg_g * (1.0 - fg_g),
                     dc_tot * in_g * (1.0 - cand_g * cand_g),
                     dh_tot * tanh_c * out_g * (1.0 - out_g))
            dc[l][:, hc] = dc_tot * fg_g
            for q, part in enumerate(parts):
                cols = slice(q * HID + j * COL, q * HID + (j + 1) * COL)
                dz[l][slot, :, cols] = part.astype(BF16)
                db_acc[l, :, cols] += jnp.sum(part.reshape(ROWS // 8, 8, COL), axis=0)
        for k in range(KT):
            prod = sum_dots([(dz[l][slot, :, n * COL:(n + 1) * COL], w[l, k, n]) for n in range(NT)])
            if k >= KT // 2:
                dr[l][:, (k - KT // 2) * COL:(k - KT // 2 + 1) * COL] = prod
            else:
                kc = slice(k * COL, (k + 1) * COL)
                total = (dy_buf[t, :, kc] if l == LOCAL - 1 else dyn[l][:, kc]) + prod
                if l > 0:
                    dyn[l - 1][:, kc] = total
                else:
                    dx_out[out_slot, :, kc] = total

    def bwd_wave(s, full):
        t_of = [STEPS + LOCAL - 2 - s - l for l in range(LOCAL)]
        slot_of = [lax.rem(t + SLOTS, SLOTS) for t in t_of]
        t_top, t_low = t_of[LOCAL - 1], t_of[0]
        out_slot = lax.rem(t_low + 2 * RING, RING)

        @pl.when(jnp.logical_and(second, both(valid(t_top, full), lax.rem(t_top, PIECE) == PIECE - 1)))
        def _():
            p = t_top // PIECE
            pltpu.make_async_copy(dy_buf.at[pl.ds(p * PIECE, PIECE)], dy_buf.at[pl.ds(p * PIECE, PIECE)], din_sem.at[p]).wait()

        @pl.when(both(valid(t_top, full), first))
        def _():
            dy_copy(t_top, 0).wait_recv()

        for l in range(LOCAL):
            t, slot = t_of[l], slot_of[l]

            @guard(True if full else jnp.logical_and(t >= 0, t < STEPS - SLOTS))
            def _():
                rec_read(l, t, slot).wait()
                dz_write(l, t + SLOTS, slot).wait()

        @pl.when(jnp.logical_and(t_low >= 0, t_low < STEPS - RING))
        def _():
            @pl.when(second)
            def _():
                dy_copy(t_low + RING, out_slot).wait_send()

            @pl.when(first)
            def _():
                home_copy(t_low + RING, out_slot).wait_send()
                own_copy(t_low + RING, out_slot).wait()

        for l in range(LOCAL):
            if full:
                bwd_cell(l, t_of[l], slot_of[l])
            else:
                @pl.when(valid(t_of[l], False))
                def _():
                    bwd_cell(l, t_of[l], slot_of[l])

        for l in range(LOCAL):
            t, slot = t_of[l], slot_of[l]

            @pl.when(both(valid(t, full), t >= SLOTS))
            def _():
                rec_read(l, t - SLOTS, slot).start()

            @guard(valid(t, full))
            def _():
                dz_write(l, t, slot).start()

        @pl.when(both(valid(t_low, full), second))
        def _():
            dy_copy(t_low, out_slot).start()

        @pl.when(both(valid(t_low, full), first))
        def _():
            home_copy(t_low, out_slot).start()
            own_copy(t_low, out_slot).start()

    run_waves(bwd_wave, 0, LOCAL - 1 + SLOTS, False)
    run_waves(bwd_wave, LOCAL - 1 + SLOTS, STEPS, True)
    run_waves(bwd_wave, STEPS, STEPS + LOCAL - 1, False)

    for l in range(LOCAL):
        db_sum[l:l + 1, :] = jnp.sum(db_acc[l], axis=0, keepdims=True)
    db_local = pltpu.make_async_copy(db_sum, db_hbm.at[core], db_sem.at[0])
    db_remote = pltpu.make_async_remote_copy(db_sum, db_hbm.at[core], db_sem.at[1], db_sem.at[2], device_id=partner, device_id_type=MESH)
    db_local.start()
    db_remote.start()

    for p in range(PIECES):
        gathered(x_piece, p, 0)
        gathered(d_piece, p, 1)
    for l in range(LOCAL):
        for t in range(SLOTS):
            dz_write(l, t, t).wait()

    @pl.when(first)
    def _():
        for s in range(RING):
            y_copy(STEPS - RING + s, s).wait_send()
            home_copy(s, s).wait_send()
            own_copy(s, s).wait()

    @pl.when(second)
    def _():
        for s in range(RING):
            dy_copy(s, s).wait_send()
        for t in range(STEPS):
            home_copy(t, 0).wait_recv()

    db_local.wait()
    db_remote.wait()


def recurrence_entry(n_data, *refs):
    ins, outs, rest = refs[:4], refs[4:9], list(refs[9:])
    take = lambda count: [rest.pop(0) for _ in range(count)]
    w, x_buf, dy_buf = take(3)
    lhs, hn, xn, cs, rec = take(4), take(4), take(3), take(4), take(4)
    y_out, = take(1)
    dz, dyn, dr, dc = take(4), take(3), take(4), take(4)
    dx_out, db_acc, db_sum = take(3)
    recurrence_kernel(n_data, *ins, *outs, w, x_buf, dy_buf, lhs, hn, xn, cs, rec, y_out, dz, dyn, dr, dc, dx_out, db_acc, db_sum, *rest)


def weight_kernel(n_data, xh_hbm, dz, dw_hbm, xh, stage, xh_sem, local_sem, send_sem, recv_sem):
    rep, data = lax.axis_index('rep'), lax.axis_index('data')
    core = lax.rem(data, 2)
    partner = {'rep': rep, 'data': data + 1 - 2 * core}
    i = pl.program_id(0)
    total = LOCAL * NT
    slot = lax.rem(i, 2)

    def out(step):
        return dw_hbm.at[core * LOCAL + step // NT, :, pl.ds(pl.multiple_of(lax.rem(step, NT) * COL, COL), COL)]

    def near(step, slot):
        return pltpu.make_async_copy(stage.at[slot], out(step), local_sem.at[slot])

    def far(step, slot):
        return pltpu.make_async_remote_copy(stage.at[slot], out(step), send_sem.at[slot], recv_sem.at[step], device_id=partner, device_id_type=MESH)

    layer, n = i // NT, lax.rem(i, NT)
    part = STEPS * ROWS // NT

    def load(layer, p):
        rows = pl.ds(pl.multiple_of(p * part, part), part)
        return pltpu.make_async_copy(xh_hbm.at[layer, rows], xh.at[lax.rem(layer, 2), rows], xh_sem.at[lax.rem(layer, 2), p])

    @pl.when(i == 0)
    def _():
        for p in range(NT):
            load(0, p).start()

    @pl.when(n == 0)
    def _():
        for p in range(NT):
            load(layer, p).wait()

    @pl.when(layer + 1 < LOCAL)
    def _():
        load(layer + 1, n).start()

    @pl.when(i >= 2)
    def _():
        near(i - 2, slot).wait()
        far(i - 2, slot).wait_send()

    stage[slot] = lax.dot_general(xh[lax.rem(layer, 2)], dz[0], (((0,), (0,)), ((), ())), preferred_element_type=F32)
    near(i, slot).start()
    far(i, slot).start()

    @pl.when(i == total - 1)
    def _():
        for back in range(2):
            near(total - 2 + back, back).wait()
            far(total - 2 + back, back).wait_send()
        for step in range(total):
            far(step, 0).wait_recv()


def solution(mesh):
    batch_axes = tuple(mesh.axis_names)
    n_data = mesh.shape['data']
    hbm = pl.BlockSpec(memory_space=pl.ANY)
    dma = pltpu.SemaphoreType.DMA

    def device_step(x_in, d_out, weights, biases):
        x_seq = jnp.swapaxes(x_in, 0, 1)
        d_seq = jnp.swapaxes(d_out, 0, 1)
        plane = lambda dtype: pltpu.VMEM((ROWS, HID), dtype)
        xh, dz, dx, db, _ = pl.pallas_call(
            functools.partial(recurrence_entry, n_data),
            out_shape=(jax.ShapeDtypeStruct((LOCAL, STEPS, ROWS, 2 * HID), BF16),
                       jax.ShapeDtypeStruct((LOCAL, STEPS, ROWS, GATES), BF16),
                       jax.ShapeDtypeStruct((STEPS, OWN, HID), F32),
                       jax.ShapeDtypeStruct((2, LOCAL, GATES), F32),
                       jax.ShapeDtypeStruct((LOCAL, STEPS, ROWS, REC), F32)),
            in_specs=[hbm, hbm, hbm, pl.BlockSpec(memory_space=pltpu.VMEM)],
            out_specs=(hbm,) * 5,
            scratch_shapes=[
                pltpu.VMEM((LOCAL, KT, NT, COL, COL), BF16),
                pltpu.VMEM((STEPS, ROWS, HID), BF16),
                pltpu.VMEM((STEPS, ROWS, HID), F32),
                *[pltpu.VMEM((SLOTS, ROWS, 2 * HID), BF16)] * 4,
                *[plane(BF16)] * 4,
                *[plane(BF16)] * 3,
                *[plane(F32)] * 4,
                *[pltpu.VMEM((SLOTS, ROWS, REC), F32)] * 4,
                pltpu.VMEM((RING, ROWS, HID), BF16),
                *[pltpu.VMEM((SLOTS, ROWS, GATES), BF16)] * 4,
                *[plane(F32)] * 3,
                *[plane(F32)] * 4,
                *[plane(F32)] * 4,
                pltpu.VMEM((RING, ROWS, HID), F32),
                pltpu.VMEM((LOCAL, 8, GATES), F32),
                pltpu.VMEM((LOCAL, GATES), F32),
                dma((LOCAL,)), dma((STEPS,)), dma((PIECES,)), dma((PIECES, CHIPS)), dma((RING,)), dma((LOCAL, SLOTS)), dma((LOCAL, SLOTS)), dma((LOCAL, SLOTS)),
                dma((STEPS,)), dma((PIECES,)), dma((PIECES, CHIPS)), dma((LOCAL, SLOTS)), dma((RING,)), dma((RING,)), dma((STEPS,)), dma((3,)),
            ],
            compiler_params=pltpu.CompilerParams(has_side_effects=True, vmem_limit_bytes=66000000),
        )(x_seq, d_seq, weights, biases)
        dw = pl.pallas_call(
            functools.partial(weight_kernel, n_data),
            out_shape=jax.ShapeDtypeStruct((2 * LOCAL, 2 * HID, GATES), F32),
            grid=(LOCAL * NT,),
            in_specs=[hbm,
                      pl.BlockSpec((1, STEPS * ROWS, COL), lambda i: (i // NT, 0, lax.rem(i, NT)))],
            out_specs=hbm,
            scratch_shapes=[pltpu.VMEM((2, STEPS * ROWS, 2 * HID), BF16), pltpu.VMEM((2, 2 * HID, COL), F32), dma((2, NT)), dma((2,)), dma((2,)), dma((LOCAL * NT,))],
            compiler_params=pltpu.CompilerParams(has_side_effects=True, vmem_limit_bytes=60000000),
        )(xh.reshape(LOCAL, STEPS * ROWS, 2 * HID), dz.reshape(LOCAL, STEPS * ROWS, GATES))
        return dw, db.reshape(2 * LOCAL, GATES), jnp.swapaxes(dx, 0, 1)

    return jax.shard_map(device_step, mesh=mesh,
                         in_specs=(P(batch_axes), P(batch_axes), P(), P()),
                         out_specs=(P(), P(), P(batch_axes)), check_vma=False)
```

```python
import functools

import jax
import jax.numpy as jnp
from jax import lax
from jax.experimental import pallas as pl
from jax.experimental.pallas import tpu as pltpu
from jax.sharding import PartitionSpec as P

HID = 512
GATES = 4 * HID
ROWS = 128
OWN = 16
STEPS = 32
LOCAL = 4
CHIPS = 4
PIECE = 4
PIECES = STEPS // PIECE
COL = 256
KT = 2 * HID // COL
NT = GATES // COL
REC = 5 * HID
RING = 4
SLOTS = 2
F32 = jnp.float32
BF16 = jnp.bfloat16
MESH = pl.DeviceIdType.MESH


def dot(a, b):
    return jnp.dot(a, b, preferred_element_type=F32)


def sum_dots(pairs):
    total = None
    for a, b in pairs:
        part = dot(a, b)
        total = part if total is None else total + part
    return total


def recurrence_kernel(n_data, x_hbm, dout_hbm, w_hbm, bias,
                      xh_hbm, dz_hbm, dx_hbm, db_hbm, rec_hbm,
                      w, x_buf, dy_buf, lhs, hn, xn, cs, rec, y_out, dz, dyn, dr, dc, dx_out, db_acc, db_sum,
                      w_sem, x_sem, xin_sem, xin_send, y_send, lhs_sem, rec_wsem, rec_rsem, dy_sem, din_sem, din_send,
                      dz_sem, dx_send, home_sem, dx_recv, db_sem):
    rep, data = lax.axis_index('rep'), lax.axis_index('data')
    core = lax.rem(data, 2)
    chip = rep * (n_data // 2) + data // 2
    me = 2 * chip + core
    first, second = core == 0, core == 1
    partner = {'rep': rep, 'data': data + 1 - 2 * core}
    my_rows = pl.ds(pl.multiple_of(me * OWN, OWN), OWN)

    def place(dev):
        return {'rep': dev // n_data, 'data': dev % n_data}

    def w_copy(l, k, n):
        return pltpu.make_async_copy(w_hbm.at[core * LOCAL + l, pl.ds(k * COL, COL), pl.ds(n * COL, COL)], w[l].at[k, n], w_sem.at[l])

    def x_piece(p, dev, remote):
        src, dst = x_hbm.at[pl.ds(p * PIECE, PIECE)], x_buf.at[pl.ds(p * PIECE, PIECE), my_rows]
        if remote:
            return pltpu.make_async_remote_copy(src, dst, xin_send.at[p, dev // 2], xin_sem.at[p], device_id=place(dev), device_id_type=MESH)
        return pltpu.make_async_copy(src, dst, xin_sem.at[p])

    def d_piece(p, dev, remote):
        src, dst = dout_hbm.at[pl.ds(p * PIECE, PIECE)], dy_buf.at[pl.ds(p * PIECE, PIECE), my_rows]
        if remote:
            return pltpu.make_async_remote_copy(src, dst, din_send.at[p, dev // 2], din_sem.at[p], device_id=place(dev), device_id_type=MESH)
        return pltpu.make_async_copy(src, dst, din_sem.at[p])

    def gather(piece, p, which):
        for dev in range(which, 2 * CHIPS, 2):
            @pl.when(me == dev)
            def _():
                piece(p, dev, False).start()

            @pl.when(me != dev)
            def _():
                piece(p, dev, True).start()

    def gathered(piece, p, which):
        for dev in range(which, 2 * CHIPS, 2):
            @pl.when(me != dev)
            def _():
                piece(p, dev, True).wait_send()

    gather(x_piece, 0, 0)
    for l in range(LOCAL):
        for k in range(KT):
            for n in range(NT):
                w_copy(l, k, n).start()
        if l == 0:
            gather(x_piece, 1, 0)

    for l in range(LOCAL):
        hn[l][...] = jnp.zeros((ROWS, HID), BF16)
        cs[l][...] = jnp.zeros((ROWS, HID), F32)

    def y_copy(t, slot):
        return pltpu.make_async_remote_copy(y_out.at[slot], x_buf.at[t], y_send.at[slot], x_sem.at[t], device_id=partner, device_id_type=MESH)

    def lhs_write(l, t, slot):
        return pltpu.make_async_copy(lhs[l].at[slot], xh_hbm.at[l, t], lhs_sem.at[l, slot])

    def rec_write(l, t, slot):
        return pltpu.make_async_copy(rec[l].at[slot], rec_hbm.at[l, t], rec_wsem.at[l, slot])

    def guard(cond):
        if isinstance(cond, bool):
            return (lambda f: f()) if cond else (lambda f: None)
        return pl.when(cond)

    def valid(t, full):
        return True if full else jnp.logical_and(t >= 0, t < STEPS)

    def both(a, b):
        return b if a is True else jnp.logical_and(a, b)

    def fwd_cell(l, t, slot):
        for j in range(HID // COL):
            hc = slice(j * COL, (j + 1) * COL)
            z = []
            for q in range(4):
                n = q * (HID // COL) + j
                z.append(sum_dots([(lhs[l][slot, :, k * COL:(k + 1) * COL], w[l][k, n]) for k in range(KT)])
                         + bias[pl.ds(core * LOCAL + l, 1), n * COL:(n + 1) * COL])
            in_g, fg_g, cand_g, out_g = jax.nn.sigmoid(z[0]), jax.nn.sigmoid(z[1]), jnp.tanh(z[2]), jax.nn.sigmoid(z[3])
            c_prev = cs[l][:, hc]
            for q, value in enumerate((in_g, fg_g, cand_g, out_g, c_prev)):
                rec[l][slot, :, q * HID + j * COL:q * HID + (j + 1) * COL] = value
            c_new = fg_g * c_prev + in_g * cand_g
            h_new = out_g * jnp.tanh(c_new)
            cs[l][:, hc] = c_new
            hn[l][:, hc] = h_new.astype(BF16)
            y_new = (h_new + lhs[l][slot, :, hc].astype(F32)).astype(BF16)
            if l < LOCAL - 1:
                xn[l][:, hc] = y_new
            else:
                y_out[lax.rem(t, RING), :, hc] = y_new

    def fwd_wave(s, full):
        t_of = [s - l for l in range(LOCAL)]
        slot_of = [lax.rem(t + SLOTS, SLOTS) for t in t_of]

        @pl.when(jnp.logical_and(first, both(valid(s, full), lax.rem(s, PIECE) == 0)))
        def _():
            p = s // PIECE
            pltpu.make_async_copy(x_buf.at[pl.ds(p * PIECE, PIECE)], x_buf.at[pl.ds(p * PIECE, PIECE)], xin_sem.at[p]).wait()

        @pl.when(both(valid(s, full), second))
        def _():
            y_copy(s, 0).wait_recv()

        if not full:
            for l in range(LOCAL):
                @pl.when(s == l)
                def _():
                    pltpu.make_async_copy(w[l], w[l], w_sem.at[l]).wait()

        for l in range(LOCAL):
            t, slot = t_of[l], slot_of[l]

            @pl.when(jnp.logical_and(t >= SLOTS, t < STEPS))
            def _():
                lhs_write(l, t - SLOTS, slot).wait()
                rec_write(l, t - SLOTS, slot).wait()

        t_top = t_of[LOCAL - 1]

        @pl.when(jnp.logical_and(first, jnp.logical_and(t_top >= RING, t_top < STEPS)))
        def _():
            y_copy(t_top - RING, lax.rem(t_top, RING)).wait_send()

        def assemble(l):
            lhs[l][slot_of[l], :, :HID] = x_buf[t_of[0]] if l == 0 else xn[l - 1][...]
            lhs[l][slot_of[l], :, HID:] = hn[l][...]

        if full:
            for l in range(LOCAL):
                assemble(l)
            for l in range(LOCAL):
                fwd_cell(l, t_of[l], slot_of[l])
        else:
            for l in reversed(range(LOCAL)):
                @pl.when(valid(t_of[l], False))
                def _():
                    assemble(l)
                    fwd_cell(l, t_of[l], slot_of[l])

        for l in range(LOCAL):
            t, slot = t_of[l], slot_of[l]

            @guard(valid(t, full))
            def _():
                lhs_write(l, t, slot).start()

            @pl.when(both(valid(t, full), t < STEPS - SLOTS))
            def _():
                rec_write(l, t, slot).start()

        @pl.when(both(valid(t_top, full), first))
        def _():
            y_copy(t_top, lax.rem(t_top, RING)).start()

        turn_of = s // 2

        @pl.when(jnp.logical_and(lax.rem(s, 2) == 0, turn_of < PIECES - 2))
        def _():
            gather(x_piece, turn_of + 2, 0)

        @pl.when(jnp.logical_and(lax.rem(s, 2) == 0, jnp.logical_and(turn_of >= PIECES - 2, turn_of < 2 * PIECES - 2)))
        def _():
            gather(d_piece, 2 * PIECES - 3 - turn_of, 1)

    def run_waves(wave, lo, hi, full):
        def body(s, carry):
            wave(s, full)
            return carry
        lax.fori_loop(lo, hi, body, 0)

    run_waves(fwd_wave, 0, LOCAL, False)
    run_waves(fwd_wave, LOCAL, STEPS, True)
    run_waves(fwd_wave, STEPS, STEPS + LOCAL - 1, False)

    def turn(i, carry):
        k, n = i // (NT // 2), 2 * lax.rem(i, NT // 2)
        for l in range(LOCAL):
            left, right = w[l][k, n].T, w[l][k, n + 1].T
            w[l][k, n] = left
            w[l][k, n + 1] = right
        return carry

    lax.fori_loop(0, KT * NT // 2, turn, 0)

    for l in range(LOCAL):
        for t in range(STEPS - SLOTS, STEPS):
            lhs_write(l, t, t % SLOTS).wait()

    def rec_read(l, t, slot):
        return pltpu.make_async_copy(rec_hbm.at[l, t], rec[l].at[slot], rec_rsem.at[l, slot])

    def dz_write(l, t, slot):
        return pltpu.make_async_copy(dz[l].at[slot], dz_hbm.at[l, t], dz_sem.at[l, slot])

    def dy_copy(t, slot):
        return pltpu.make_async_remote_copy(dx_out.at[slot], dy_buf.at[t], dx_send.at[slot], dy_sem.at[t], device_id=partner, device_id_type=MESH)

    def home_copy(t, slot):
        rows = pl.ds(pl.multiple_of((2 * chip + 1) * OWN, OWN), OWN)
        return pltpu.make_async_remote_copy(dx_out.at[slot, rows], dx_hbm.at[t], dx_send.at[slot], dx_recv.at[t], device_id=partner, device_id_type=MESH)

    def own_copy(t, slot):
        return pltpu.make_async_copy(dx_out.at[slot, my_rows], dx_hbm.at[t], home_sem.at[slot])

    for l in range(LOCAL):
        dr[l][...] = jnp.zeros((ROWS, HID), F32)
        dc[l][...] = jnp.zeros((ROWS, HID), F32)
    db_acc[...] = jnp.zeros((LOCAL, 8, GATES), F32)

    def bwd_cell(l, t, slot):
        out_slot = lax.rem(t, RING)
        for j in range(HID // COL):
            hc = slice(j * COL, (j + 1) * COL)
            in_g, fg_g, cand_g, out_g, c_prev = (rec[l][slot, :, q * HID + j * COL:q * HID + (j + 1) * COL] for q in range(5))
            tanh_c = jnp.tanh(fg_g * c_prev + in_g * cand_g)
            dy = dy_buf[t, :, hc] if l == LOCAL - 1 else dyn[l][:, hc]
            dh_tot = dy + dr[l][:, hc]
            dc_tot = dc[l][:, hc] + dh_tot * out_g * (1.0 - tanh_c * tanh_c)
            parts = (dc_tot * cand_g * in_g * (1.0 - in_g),
                     dc_tot * c_prev * fg_g * (1.0 - fg_g),
                     dc_tot * in_g * (1.0 - cand_g * cand_g),
                     dh_tot * tanh_c * out_g * (1.0 - out_g))
            dc[l][:, hc] = dc_tot * fg_g
            for q, part in enumerate(parts):
                cols = slice(q * HID + j * COL, q * HID + (j + 1) * COL)
                dz[l][slot, :, cols] = part.astype(BF16)
                db_acc[l, :, cols] += jnp.sum(part.reshape(ROWS // 8, 8, COL), axis=0)
        for k in range(KT):
            prod = sum_dots([(dz[l][slot, :, n * COL:(n + 1) * COL], w[l][k, n]) for n in range(NT)])
            if k >= KT // 2:
                dr[l][:, (k - KT // 2) * COL:(k - KT // 2 + 1) * COL] = prod
            else:
                kc = slice(k * COL, (k + 1) * COL)
                total = (dy_buf[t, :, kc] if l == LOCAL - 1 else dyn[l][:, kc]) + prod
                if l > 0:
                    dyn[l - 1][:, kc] = total
                else:
                    dx_out[out_slot, :, kc] = total

    def bwd_wave(s, full):
        t_of = [STEPS + LOCAL - 2 - s - l for l in range(LOCAL)]
        slot_of = [lax.rem(t + SLOTS, SLOTS) for t in t_of]
        t_top, t_low = t_of[LOCAL - 1], t_of[0]
        out_slot = lax.rem(t_low + 2 * RING, RING)

        @pl.when(jnp.logical_and(second, both(valid(t_top, full), lax.rem(t_top, PIECE) == PIECE - 1)))
        def _():
            p = t_top // PIECE
            pltpu.make_async_copy(dy_buf.at[pl.ds(p * PIECE, PIECE)], dy_buf.at[pl.ds(p * PIECE, PIECE)], din_sem.at[p]).wait()

        @pl.when(both(valid(t_top, full), first))
        def _():
            dy_copy(t_top, 0).wait_recv()

        for l in range(LOCAL):
            t, slot = t_of[l], slot_of[l]

            @pl.when(jnp.logical_and(t >= 0, t < STEPS - SLOTS))
            def _():
                rec_read(l, t, slot).wait()
                dz_write(l, t + SLOTS, slot).wait()

        @pl.when(jnp.logical_and(t_low >= 0, t_low < STEPS - RING))
        def _():
            @pl.when(second)
            def _():
                dy_copy(t_low + RING, out_slot).wait_send()

            @pl.when(first)
            def _():
                home_copy(t_low + RING, out_slot).wait_send()
                own_copy(t_low + RING, out_slot).wait()

        for l in range(LOCAL):
            if full:
                bwd_cell(l, t_of[l], slot_of[l])
            else:
                @pl.when(valid(t_of[l], False))
                def _():
                    bwd_cell(l, t_of[l], slot_of[l])

        for l in range(LOCAL):
            t, slot = t_of[l], slot_of[l]

            @pl.when(both(valid(t, full), t >= SLOTS))
            def _():
                rec_read(l, t - SLOTS, slot).start()

            @guard(valid(t, full))
            def _():
                dz_write(l, t, slot).start()

        @pl.when(both(valid(t_low, full), second))
        def _():
            dy_copy(t_low, out_slot).start()

        @pl.when(both(valid(t_low, full), first))
        def _():
            home_copy(t_low, out_slot).start()
            own_copy(t_low, out_slot).start()

    run_waves(bwd_wave, 0, LOCAL - 1, False)
    run_waves(bwd_wave, LOCAL - 1, STEPS, True)
    run_waves(bwd_wave, STEPS, STEPS + LOCAL - 1, False)

    for l in range(LOCAL):
        db_sum[l:l + 1, :] = jnp.sum(db_acc[l], axis=0, keepdims=True)
    db_local = pltpu.make_async_copy(db_sum, db_hbm.at[core], db_sem.at[0])
    db_remote = pltpu.make_async_remote_copy(db_sum, db_hbm.at[core], db_sem.at[1], db_sem.at[2], device_id=partner, device_id_type=MESH)
    db_local.start()
    db_remote.start()

    for p in range(PIECES):
        gathered(x_piece, p, 0)
        gathered(d_piece, p, 1)
    for l in range(LOCAL):
        for t in range(SLOTS):
            dz_write(l, t, t).wait()

    @pl.when(first)
    def _():
        for s in range(RING):
            y_copy(STEPS - RING + s, s).wait_send()
            home_copy(s, s).wait_send()
            own_copy(s, s).wait()

    @pl.when(second)
    def _():
        for s in range(RING):
            dy_copy(s, s).wait_send()
        for t in range(STEPS):
            home_copy(t, 0).wait_recv()

    db_local.wait()
    db_remote.wait()


def recurrence_entry(n_data, *refs):
    ins, outs, rest = refs[:4], refs[4:9], list(refs[9:])
    take = lambda count: [rest.pop(0) for _ in range(count)]
    w = take(4)
    x_buf, dy_buf = take(2)
    lhs, hn, xn, cs, rec = take(4), take(4), take(3), take(4), take(4)
    y_out, = take(1)
    dz, dyn, dr, dc = take(4), take(3), take(4), take(4)
    dx_out, db_acc, db_sum = take(3)
    recurrence_kernel(n_data, *ins, *outs, w, x_buf, dy_buf, lhs, hn, xn, cs, rec, y_out, dz, dyn, dr, dc, dx_out, db_acc, db_sum, *rest)


def weight_kernel(n_data, xh_hbm, dz, dw_hbm, xh, stage, xh_sem, local_sem, send_sem, recv_sem):
    rep, data = lax.axis_index('rep'), lax.axis_index('data')
    core = lax.rem(data, 2)
    partner = {'rep': rep, 'data': data + 1 - 2 * core}
    i = pl.program_id(0)
    total = LOCAL * NT
    slot = lax.rem(i, 2)

    def out(step):
        return dw_hbm.at[core * LOCAL + step // NT, :, pl.ds(pl.multiple_of(lax.rem(step, NT) * COL, COL), COL)]

    def near(step, slot):
        return pltpu.make_async_copy(stage.at[slot], out(step), local_sem.at[slot])

    def far(step, slot):
        return pltpu.make_async_remote_copy(stage.at[slot], out(step), send_sem.at[slot], recv_sem.at[step], device_id=partner, device_id_type=MESH)

    layer, n = i // NT, lax.rem(i, NT)
    part = STEPS * ROWS // NT

    def load(layer, p):
        rows = pl.ds(pl.multiple_of(p * part, part), part)
        return pltpu.make_async_copy(xh_hbm.at[layer, rows], xh.at[lax.rem(layer, 2), rows], xh_sem.at[lax.rem(layer, 2), p])

    @pl.when(i == 0)
    def _():
        for p in range(NT):
            load(0, p).start()

    @pl.when(n == 0)
    def _():
        for p in range(NT):
            load(layer, p).wait()

    @pl.when(layer + 1 < LOCAL)
    def _():
        load(layer + 1, n).start()

    @pl.when(i >= 2)
    def _():
        near(i - 2, slot).wait()
        far(i - 2, slot).wait_send()

    stage[slot] = lax.dot_general(xh[lax.rem(layer, 2)], dz[0], (((0,), (0,)), ((), ())), preferred_element_type=F32)
    near(i, slot).start()
    far(i, slot).start()

    @pl.when(i == total - 1)
    def _():
        for back in range(2):
            near(total - 2 + back, back).wait()
            far(total - 2 + back, back).wait_send()
        for step in range(total):
            far(step, 0).wait_recv()


def solution(mesh):
    batch_axes = tuple(mesh.axis_names)
    n_data = mesh.shape['data']
    hbm = pl.BlockSpec(memory_space=pl.ANY)
    dma = pltpu.SemaphoreType.DMA

    def device_step(x_in, d_out, weights, biases):
        x_seq = jnp.swapaxes(x_in, 0, 1)
        d_seq = jnp.swapaxes(d_out, 0, 1)
        plane = lambda dtype: pltpu.VMEM((ROWS, HID), dtype)
        xh, dz, dx, db, _ = pl.pallas_call(
            functools.partial(recurrence_entry, n_data),
            out_shape=(jax.ShapeDtypeStruct((LOCAL, STEPS, ROWS, 2 * HID), BF16),
                       jax.ShapeDtypeStruct((LOCAL, STEPS, ROWS, GATES), BF16),
                       jax.ShapeDtypeStruct((STEPS, OWN, HID), F32),
                       jax.ShapeDtypeStruct((2, LOCAL, GATES), F32),
                       jax.ShapeDtypeStruct((LOCAL, STEPS, ROWS, REC), F32)),
            in_specs=[hbm, hbm, hbm, pl.BlockSpec(memory_space=pltpu.VMEM)],
            out_specs=(hbm,) * 5,
            scratch_shapes=[
                *[pltpu.VMEM((KT, NT, COL, COL), BF16)] * 4,
                pltpu.VMEM((STEPS, ROWS, HID), BF16),
                pltpu.VMEM((STEPS, ROWS, HID), F32),
                *[pltpu.VMEM((SLOTS, ROWS, 2 * HID), BF16)] * 4,
                *[plane(BF16)] * 4,
                *[plane(BF16)] * 3,
                *[plane(F32)] * 4,
                *[pltpu.VMEM((SLOTS, ROWS, REC), F32)] * 4,
                pltpu.VMEM((RING, ROWS, HID), BF16),
                *[pltpu.VMEM((SLOTS, ROWS, GATES), BF16)] * 4,
                *[plane(F32)] * 3,
                *[plane(F32)] * 4,
                *[plane(F32)] * 4,
                pltpu.VMEM((RING, ROWS, HID), F32),
                pltpu.VMEM((LOCAL, 8, GATES), F32),
                pltpu.VMEM((LOCAL, GATES), F32),
                dma((LOCAL,)), dma((STEPS,)), dma((PIECES,)), dma((PIECES, CHIPS)), dma((RING,)), dma((LOCAL, SLOTS)), dma((LOCAL, SLOTS)), dma((LOCAL, SLOTS)),
                dma((STEPS,)), dma((PIECES,)), dma((PIECES, CHIPS)), dma((LOCAL, SLOTS)), dma((RING,)), dma((RING,)), dma((STEPS,)), dma((3,)),
            ],
            compiler_params=pltpu.CompilerParams(has_side_effects=True, vmem_limit_bytes=66000000),
        )(x_seq, d_seq, weights, biases)
        dw = pl.pallas_call(
            functools.partial(weight_kernel, n_data),
            out_shape=jax.ShapeDtypeStruct((2 * LOCAL, 2 * HID, GATES), F32),
            grid=(LOCAL * NT,),
            in_specs=[hbm,
                      pl.BlockSpec((1, STEPS * ROWS, COL), lambda i: (i // NT, 0, lax.rem(i, NT)))],
            out_specs=hbm,
            scratch_shapes=[pltpu.VMEM((2, STEPS * ROWS, 2 * HID), BF16), pltpu.VMEM((2, 2 * HID, COL), F32), dma((2, NT)), dma((2,)), dma((2,)), dma((LOCAL * NT,))],
            compiler_params=pltpu.CompilerParams(has_side_effects=True, vmem_limit_bytes=60000000),
        )(xh.reshape(LOCAL, STEPS * ROWS, 2 * HID), dz.reshape(LOCAL, STEPS * ROWS, GATES))
        return dw, db.reshape(2 * LOCAL, GATES), jnp.swapaxes(dx, 0, 1)

    return jax.shard_map(device_step, mesh=mesh,
                         in_specs=(P(batch_axes), P(batch_axes), P(), P()),
                         out_specs=(P(), P(), P(batch_axes)), check_vma=False)
```
